32 devices in a mesh: shard: 32 (over z, y, x, core).
Axes of the slice: x: 2, y: 2, z: 4, core: 2. Of those that a mesh axis runs over, the one named last changes fastest.
Arguments:
- picked_rows: int32 [1024, 8], P('shard'), may hold values from 0 to 16383
- main_table: float32 [16384, 128], P('shard'), may hold values from -6 to 6
- dense_part: float32 [1024, 128], P('shard'), may hold values from -6 to 6
- small_ids: int32 [1024], P('shard'), may hold values from 0 to 127
- small_table: float32 [128, 128], P('shard'), may hold values from -6 to 6
- scale_ids: int32 [1024], P('shard'), may hold values from 0 to 127
Outputs:
- features: float32 [1024, 3, 128], P('shard')
The draws below stay inside these ranges and needn't reach their ends.
All inputs are finite; a program needn't handle non-finite values.
Results may differ from the reference program's by a relative error of at most 0.0003.
Values sent between devices are 32-bit elements.
A program may use at most 64 MiB of HBM per device.

```python
import math
import jax
import jax.numpy as jnp
import numpy as np

EXAMPLES = 1024
FEATURES = 128
PICKS = 8
BIG_ROWS = 16384
SMALL_ROWS = 128


def place_ends(array, key, low, top_value):
    index_at = [jax.random.randint(jax.random.fold_in(key, axis), (), 0, length) for axis, length in enumerate(array.shape)]
    main_axis = array.shape.index(max(array.shape))
    beside = index_at[:main_axis] + [(index_at[main_axis] + 1) % array.shape[main_axis]] + index_at[main_axis + 1:]
    return array.at[tuple(index_at)].set(low).at[tuple(beside)].set(top_value)


def levels(key, dims, shards, least, top_value):
    gain, own = 1.0, jax.random.fold_in(key, 6)
    for position, shards_of in shards:
        steps = jnp.exp(jax.random.uniform(jax.random.fold_in(own, position), (shards_of,), jnp.float32, least / len(shards), top_value / len(shards)))
        gain = gain * jnp.repeat(steps, dims[position] // shards_of).reshape([-1 if axis == position else 1 for axis in range(len(dims))])
    return gain


def rank_bounds(count, lean):
    portions = [(1 << 20) // math.isqrt(standing ** lean) + 1 for standing in range(1, count + 1)]
    width = 1 + sum(portions) // (1 << 30)
    return np.cumsum(np.array([max(1, weight // width) for weight in portions]))


def skewed_ids(rng, extent, number_of, skew):
    listing = rank_bounds(number_of, skew)
    lot = jax.random.randint(jax.random.fold_in(rng, 1), extent, 0, int(listing[number_of - 1]))
    grade = jnp.searchsorted(jnp.asarray(listing, jnp.int32), lot, side="right")
    return jax.random.permutation(jax.random.fold_in(rng, 2), number_of)[grade].astype(jnp.int32)


def noise(rng, dims, scale, limit, cuts=(), dtype=jnp.bfloat16):
    values = scale * jax.random.normal(rng, dims, jnp.float32)
    if cuts:
        values = values * levels(rng, dims, cuts, -0.22, 0.18)
    return jnp.clip(values, -limit, limit).astype(dtype)


def setup_inputs(seed: int = 0) -> dict:
    key_of = jax.random.split(jax.random.key(seed), 7)
    return {
        "picked_rows": place_ends(skewed_ids(key_of[0], (EXAMPLES, PICKS), BIG_ROWS, 1), jax.random.fold_in(key_of[0], 3), 0, BIG_ROWS - 1).astype(jnp.int32),
        "main_table": noise(key_of[1], (BIG_ROWS, FEATURES), 1.0, 6.0, ((0, 32),), jnp.float32),
        "dense_part": noise(key_of[2], (EXAMPLES, FEATURES), 1.0, 6.0, ((0, 32),), jnp.float32),
        "small_ids": place_ends(jax.random.randint(key_of[3], (EXAMPLES,), 0, SMALL_ROWS), jax.random.fold_in(key_of[3], 1), 0, SMALL_ROWS - 1).astype(jnp.int32),
        "small_table": noise(key_of[4], (SMALL_ROWS, FEATURES), 1.0, 6.0, ((0, 32),), jnp.float32),
        "scale_ids": place_ends(skewed_ids(key_of[5], (EXAMPLES,), SMALL_ROWS, 1), jax.random.fold_in(key_of[5], 3), 0, SMALL_ROWS - 1).astype(jnp.int32),
    }


def reference(picked_rows, main_table, dense_part, small_ids, small_table, scale_ids):
    pooled = jnp.sum(main_table[picked_rows].astype(jnp.float32), axis=1) * PICKS ** -0.5
    small_rows = small_table[small_ids].astype(jnp.float32)
    dense_part = dense_part * small_table[scale_ids].astype(jnp.float32)
    features = jnp.stack([dense_part * pooled, pooled * small_rows, dense_part * small_rows], axis=1)
    return features
```

```python
import functools

import jax
import jax.numpy as jnp
from jax import lax
from jax.experimental import pallas as pl
from jax.experimental.pallas import tpu as pltpu
from jax.sharding import PartitionSpec as P

MESH = pl.DeviceIdType.MESH
AXIS = "shard"
BATCH = 4


def two_terms(x):
    high = x.astype(jnp.bfloat16)
    low = (x - high.astype(jnp.float32)).astype(jnp.bfloat16)
    return high, low


def kernel(
    groups,
    picked_ref,
    table_ref,
    dense_ref,
    small_ids_ref,
    scale_ids_ref,
    small_ref,
    out_ref,
    ids_buf,
    table_buf,
    small_buf,
    weights,
    counts,
    part_buf,
    recv_buf,
    local_sem,
    pair_send,
    pair_recv,
    ids_send,
    ids_recv,
    small_send,
    small_recv,
    part_send,
    part_recv,
):
    examples, picks = picked_ref.shape
    rows = table_ref.shape[0]
    small = small_ref.shape[0]
    batch = min(BATCH, groups)
    me = lax.axis_index(AXIS)
    core = lax.rem(me, 2)
    mine = lax.div(me, 2)
    partner = mine * 2 + 1 - core

    def peer(step):
        return lax.rem(mine + step + 1, groups)

    barrier = pltpu.get_barrier_semaphore()
    pl.semaphore_signal(barrier, inc=1, device_id=(partner,), device_id_type=MESH)

    def greet(step, _):
        pl.semaphore_signal(
            barrier, inc=1, device_id=(peer(step) * 2 + core,), device_id_type=MESH
        )
        return 0

    lax.fori_loop(0, groups - 1, greet, 0)

    own_rows = table_buf.at[pl.ds(pl.multiple_of(core * rows, rows), rows)]
    own_small = small_buf.at[pl.ds(pl.multiple_of(me * small, small), small)]
    table_in = pltpu.make_async_copy(table_ref, own_rows, local_sem.at[0])
    small_in = pltpu.make_async_copy(small_ref, own_small, local_sem.at[1])
    table_in.start()
    small_in.start()
    ids_buf[mine] = jnp.transpose(picked_ref[...])
    table_in.wait()
    small_in.wait()

    pl.semaphore_wait(barrier, groups)

    def ids_copy(slot, sem, to):
        return pltpu.make_async_remote_copy(
            src_ref=ids_buf.at[slot],
            dst_ref=ids_buf.at[slot],
            send_sem=ids_send.at[sem],
            recv_sem=ids_recv.at[slot],
            device_id=(to * 2 + core,),
            device_id_type=MESH,
        )

    def send_ids(step, _):
        ids_copy(mine, step, peer(step)).start()
        return 0

    lax.fori_loop(0, groups - 1, send_ids, 0)

    def pair_copy(src, dst, sem):
        return pltpu.make_async_remote_copy(
            src_ref=src,
            dst_ref=dst,
            send_sem=pair_send.at[sem],
            recv_sem=pair_recv.at[sem],
            device_id=(partner,),
            device_id_type=MESH,
        )

    pair_small = pair_copy(own_small, own_small, 0)
    pair_small.start()
    pair_table = pair_copy(own_rows, own_rows, 1)
    pair_table.start()
    pair_small.wait()

    def small_copy(slot, sem, to):
        block = small_buf.at[pl.ds(pl.multiple_of(slot * 2 * small, 2 * small), 2 * small)]
        return pltpu.make_async_remote_copy(
            src_ref=block,
            dst_ref=block,
            send_sem=small_send.at[sem],
            recv_sem=small_recv.at[slot],
            device_id=(to * 2 + core,),
            device_id_type=MESH,
        )

    def send_small(step, _):
        small_copy(mine, step, peer(step)).start()
        return 0

    lax.fori_loop(0, groups - 1, send_small, 0)

    pair_table.wait()
    high, low = two_terms(table_buf[...])
    features = high.shape[1]
    weights[:, :features] = high
    weights[:, features:] = low

    def part_copy(step, slot, to):
        return pltpu.make_async_remote_copy(
            src_ref=part_buf.at[pl.ds(pl.multiple_of(step * examples, examples), examples)],
            dst_ref=recv_buf.at[pl.ds(pl.multiple_of(slot * examples, examples), examples)],
            send_sem=part_send.at[step],
            recv_sem=part_recv.at[slot],
            device_id=(to * 2 + core,),
            device_id_type=MESH,
        )

    first = mine * (2 * rows)
    half = 16
    row_of = lax.broadcasted_iota(jnp.int32, (half, 2 * rows), 1)

    def serve(index, _):
        for q in range(batch):
            source = peer(index * batch + q)

            @pl.when(source != mine)
            def _():
                ids_copy(source, 0, source).wait_recv()

            wanted = jnp.transpose(ids_buf[source]) - first
            for h in range(examples // half):
                block = wanted[h * half : (h + 1) * half]
                count = jnp.zeros((half, 2 * rows), jnp.int32)
                for k in range(picks):
                    count = count + (block[:, k : k + 1] == row_of).astype(jnp.int32)
                counts[pl.ds(q * examples + h * half, half), :] = count.astype(
                    jnp.float32
                ).astype(jnp.bfloat16)
        both = jnp.dot(counts[...], weights[...], preferred_element_type=jnp.float32)
        total = both[:, :features] + both[:, features:]
        part_buf[
            pl.ds(pl.multiple_of(index * batch * examples, batch * examples), batch * examples), :
        ] = total
        for q in range(batch):
            step = index * batch + q
            to = peer(step)

            @pl.when(to != mine)
            def _():
                part_copy(step, mine, to).start()

        return 0

    lax.fori_loop(0, groups // batch, serve, 0)

    def take_small(step, _):
        source = peer(step)
        small_copy(source, 0, source).wait_recv()
        return 0

    lax.fori_loop(0, groups - 1, take_small, 0)

    all_small = small_buf.shape[0]
    small_row = lax.broadcasted_iota(jnp.int32, (all_small, examples), 0)
    table = small_buf[...]
    s_high, s_rest = table.astype(jnp.bfloat16), None
    rest = table - s_high.astype(jnp.float32)
    s_mid, s_low = two_terms(rest)

    def look_up(ids):
        chosen = jnp.where(ids == small_row, 1.0, 0.0).astype(jnp.bfloat16)

        def take(values):
            return lax.dot_general(
                chosen,
                values,
                (((0,), (0,)), ((), ())),
                preferred_element_type=jnp.float32,
            )

        return take(s_high) + take(s_mid) + take(s_low)

    small_rows = look_up(small_ids_ref[...])
    dense = dense_ref[...] * look_up(scale_ids_ref[...])

    def add(step, total):
        source = lax.rem(mine + groups - 1 - step, groups)
        part_copy(0, source, source).wait_recv()
        return total + recv_buf[
            pl.ds(pl.multiple_of(source * examples, examples), examples), :
        ]

    total = lax.fori_loop(0, groups - 1, add, part_buf[(groups - 1) * examples :, :])
    pooled = total * picks ** (-0.5)
    out_ref[0] = dense * pooled
    out_ref[1] = pooled * small_rows
    out_ref[2] = dense * small_rows

    def finish(step, _):
        ids_copy(mine, step, peer(step)).wait_send()
        small_copy(mine, step, peer(step)).wait_send()
        part_copy(step, mine, peer(step)).wait_send()
        return 0

    lax.fori_loop(0, groups - 1, finish, 0)


def local(picked_rows, main_table, dense_part, small_ids, small_table, scale_ids):
    devices = lax.axis_size(AXIS)
    groups = devices // 2
    examples, picks = picked_rows.shape
    rows, features = main_table.shape
    small = small_table.shape[0]
    vmem = pl.BlockSpec(memory_space=pltpu.VMEM)
    anywhere = pl.BlockSpec(memory_space=pl.ANY)
    dma = pltpu.SemaphoreType.DMA
    result = pl.pallas_call(
        functools.partial(kernel, groups),
        out_shape=jax.ShapeDtypeStruct((3, examples, features), jnp.float32),
        in_specs=[vmem, anywhere, vmem, vmem, vmem, anywhere],
        out_specs=vmem,
        scratch_shapes=[
            pltpu.VMEM((groups, picks, examples), jnp.int32),
            pltpu.VMEM((2 * rows, features), jnp.float32),
            pltpu.VMEM((devices * small, features), jnp.float32),
            pltpu.VMEM((2 * rows, 2 * features), jnp.bfloat16),
            pltpu.VMEM((min(BATCH, groups) * examples, 2 * rows), jnp.bfloat16),
            pltpu.VMEM((groups * examples, features), jnp.float32),
            pltpu.VMEM((groups * examples, features), jnp.float32),
            dma((2,)),
            dma((2,)),
            dma((2,)),
            dma((groups,)),
            dma((groups,)),
            dma((groups,)),
            dma((groups,)),
            dma((groups,)),
            dma((groups,)),
        ],
        compiler_params=pltpu.CompilerParams(collective_id=0, has_side_effects=True),
    )(
        picked_rows,
        main_table,
        dense_part,
        small_ids.reshape(1, examples),
        scale_ids.reshape(1, examples),
        small_table,
    )
    return jnp.transpose(result, (1, 0, 2))


def solution(mesh):
    placed = (
        P("shard", None),
        P("shard", None),
        P("shard", None),
        P("shard"),
        P("shard", None),
        P("shard"),
    )
    return jax.shard_map(
        local, mesh=mesh, in_specs=placed, out_specs=P("shard", None, None), check_vma=False
    )
```

```python
import functools

import jax
import jax.numpy as jnp
from jax import lax
from jax.experimental import pallas as pl
from jax.experimental.pallas import tpu as pltpu
from jax.sharding import PartitionSpec as P

MESH = pl.DeviceIdType.MESH
AXIS = "shard"
BATCH = 4


def two_terms(x):
    high = x.astype(jnp.bfloat16)
    low = (x - high.astype(jnp.float32)).astype(jnp.bfloat16)
    return high, low


def kernel(
    groups,
    picked_ref,
    table_ref,
    dense_ref,
    small_ids_ref,
    scale_ids_ref,
    small_ref,
    out_ref,
    ids_buf,
    table_buf,
    small_buf,
    dense_buf,
    lookup_buf,
    weights,
    counts,
    part_buf,
    recv_buf,
    local_sem,
    pair_send,
    pair_recv,
    ids_send,
    ids_recv,
    small_send,
    small_recv,
    part_send,
    part_recv,
):
    picks, examples = picked_ref.shape
    rows = table_ref.shape[0]
    small = small_ref.shape[0]
    batch = min(BATCH, groups)
    me = lax.axis_index(AXIS)
    core = lax.rem(me, 2)
    mine = lax.div(me, 2)
    partner = mine * 2 + 1 - core

    def peer(step):
        return lax.rem(mine + step + 1, groups)

    barrier = pltpu.get_barrier_semaphore()
    pl.semaphore_signal(barrier, inc=1, device_id=(partner,), device_id_type=MESH)

    def greet(step, _):
        pl.semaphore_signal(
            barrier, inc=1, device_id=(peer(step) * 2 + core,), device_id_type=MESH
        )
        return 0

    lax.fori_loop(0, groups - 1, greet, 0)

    own_rows = table_buf.at[pl.ds(pl.multiple_of(core * rows, rows), rows)]
    own_small = small_buf.at[pl.ds(pl.multiple_of(me * small, small), small)]
    ids_in = pltpu.make_async_copy(picked_ref, ids_buf.at[mine], local_sem.at[2])
    ids_in.start()
    table_in = pltpu.make_async_copy(table_ref, own_rows, local_sem.at[0])
    small_in = pltpu.make_async_copy(small_ref, own_small, local_sem.at[1])
    table_in.start()
    small_in.start()
    dense_in = pltpu.make_async_copy(dense_ref, dense_buf, local_sem.at[3])
    first_in = pltpu.make_async_copy(small_ids_ref, lookup_buf.at[0], local_sem.at[4])
    second_in = pltpu.make_async_copy(scale_ids_ref, lookup_buf.at[1], local_sem.at[5])
    dense_in.start()
    first_in.start()
    second_in.start()
    ids_in.wait()
    small_in.wait()
    pl.semaphore_wait(barrier, groups)

    def ids_copy(slot, sem, to):
        return pltpu.make_async_remote_copy(
            src_ref=ids_buf.at[slot],
            dst_ref=ids_buf.at[slot],
            send_sem=ids_send.at[sem],
            recv_sem=ids_recv.at[slot],
            device_id=(to * 2 + core,),
            device_id_type=MESH,
        )

    def send_ids(step, _):
        ids_copy(mine, step, peer(step)).start()
        return 0

    lax.fori_loop(0, groups - 1, send_ids, 0)

    def pair_copy(src, dst, sem):
        return pltpu.make_async_remote_copy(
            src_ref=src,
            dst_ref=dst,
            send_sem=pair_send.at[sem],
            recv_sem=pair_recv.at[sem],
            device_id=(partner,),
            device_id_type=MESH,
        )

    pair_small = pair_copy(own_small, own_small, 0)
    pair_small.start()
    table_in.wait()
    pair_table = pair_copy(own_rows, own_rows, 1)
    pair_table.start()
    pair_small.wait()

    def small_copy(slot, sem, to):
        block = small_buf.at[pl.ds(pl.multiple_of(slot * 2 * small, 2 * small), 2 * small)]
        return pltpu.make_async_remote_copy(
            src_ref=block,
            dst_ref=block,
            send_sem=small_send.at[sem],
            recv_sem=small_recv.at[slot],
            device_id=(to * 2 + core,),
            device_id_type=MESH,
        )

    def send_small(step, _):
        small_copy(mine, step, peer(step)).start()
        return 0

    lax.fori_loop(0, groups - 1, send_small, 0)

    pair_table.wait()
    high, low = two_terms(table_buf[...])
    features = high.shape[1]
    weights[:, :features] = high
    weights[:, features:] = low

    def part_copy(step, slot, to):
        return pltpu.make_async_remote_copy(
            src_ref=part_buf.at[pl.ds(pl.multiple_of(step * examples, examples), examples)],
            dst_ref=recv_buf.at[pl.ds(pl.multiple_of(slot * examples, examples), examples)],
            send_sem=part_send.at[step],
            recv_sem=part_recv.at[slot],
            device_id=(to * 2 + core,),
            device_id_type=MESH,
        )

    first = mine * (2 * rows)
    half = 16
    row_of = lax.broadcasted_iota(jnp.int32, (half, 2 * rows), 1)

    def serve(index, _):
        for q in range(batch):
            source = peer(index * batch + q)

            @pl.when(source != mine)
            def _():
                ids_copy(source, 0, source).wait_recv()

            wanted = jnp.transpose(ids_buf[source]) - first
            for h in range(examples // half):
                block = wanted[h * half : (h + 1) * half]
                count = jnp.zeros((half, 2 * rows), jnp.int32)
                for k in range(picks):
                    count = count + (block[:, k : k + 1] == row_of).astype(jnp.int32)
                counts[pl.ds(q * examples + h * half, half), :] = count.astype(
                    jnp.float32
                ).astype(jnp.bfloat16)
        both = jnp.dot(counts[...], weights[...], preferred_element_type=jnp.float32)
        total = both[:, :features] + both[:, features:]
        part_buf[
            pl.ds(pl.multiple_of(index * batch * examples, batch * examples), batch * examples), :
        ] = total
        for q in range(batch):
            step = index * batch + q
            to = peer(step)

            @pl.when(to != mine)
            def _():
                part_copy(step, mine, to).start()

        return 0

    lax.fori_loop(0, groups // batch, serve, 0)

    def take_small(step, _):
        source = peer(step)
        small_copy(source, 0, source).wait_recv()
        return 0

    lax.fori_loop(0, groups - 1, take_small, 0)

    all_small = small_buf.shape[0]
    small_row = lax.broadcasted_iota(jnp.int32, (all_small, examples), 0)
    table = small_buf[...]
    s_high, s_rest = table.astype(jnp.bfloat16), None
    rest = table - s_high.astype(jnp.float32)
    s_mid, s_low = two_terms(rest)

    def look_up(ids):
        chosen = jnp.where(ids == small_row, 1.0, 0.0).astype(jnp.bfloat16)

        def take(values):
            return lax.dot_general(
                chosen,
                values,
                (((0,), (0,)), ((), ())),
                preferred_element_type=jnp.float32,
            )

        return take(s_high) + take(s_mid) + take(s_low)

    dense_in.wait()
    first_in.wait()
    second_in.wait()
    small_rows = look_up(lookup_buf[0])
    dense = dense_buf[...] * look_up(lookup_buf[1])

    def add(step, total):
        source = lax.rem(mine + groups - 1 - step, groups)
        part_copy(0, source, source).wait_recv()
        return total + recv_buf[
            pl.ds(pl.multiple_of(source * examples, examples), examples), :
        ]

    total = lax.fori_loop(0, groups - 1, add, part_buf[(groups - 1) * examples :, :])
    pooled = total * picks ** (-0.5)
    out_ref[0] = dense * pooled
    out_ref[1] = pooled * small_rows
    out_ref[2] = dense * small_rows

    def finish(step, _):
        ids_copy(mine, step, peer(step)).wait_send()
        small_copy(mine, step, peer(step)).wait_send()
        part_copy(step, mine, peer(step)).wait_send()
        return 0

    lax.fori_loop(0, groups - 1, finish, 0)


def local(picked_rows, main_table, dense_part, small_ids, small_table, scale_ids):
    devices = lax.axis_size(AXIS)
    groups = devices // 2
    examples, picks = picked_rows.shape
    rows, features = main_table.shape
    small = small_table.shape[0]
    vmem = pl.BlockSpec(memory_space=pltpu.VMEM)
    anywhere = pl.BlockSpec(memory_space=pl.ANY)
    dma = pltpu.SemaphoreType.DMA
    result = pl.pallas_call(
        functools.partial(kernel, groups),
        out_shape=jax.ShapeDtypeStruct((3, examples, features), jnp.float32),
        in_specs=[anywhere] * 6,
        out_specs=vmem,
        scratch_shapes=[
            pltpu.VMEM((groups, picks, examples), jnp.int32),
            pltpu.VMEM((2 * rows, features), jnp.float32),
            pltpu.VMEM((devices * small, features), jnp.float32),
            pltpu.VMEM((examples, features), jnp.float32),
            pltpu.VMEM((2, 1, examples), jnp.int32),
            pltpu.VMEM((2 * rows, 2 * features), jnp.bfloat16),
            pltpu.VMEM((min(BATCH, groups) * examples, 2 * rows), jnp.bfloat16),
            pltpu.VMEM((groups * examples, features), jnp.float32),
            pltpu.VMEM((groups * examples, features), jnp.float32),
            dma((6,)),
            dma((2,)),
            dma((2,)),
            dma((groups,)),
            dma((groups,)),
            dma((groups,)),
            dma((groups,)),
            dma((groups,)),
            dma((groups,)),
        ],
        compiler_params=pltpu.CompilerParams(collective_id=0, has_side_effects=True),
    )(
        jnp.transpose(picked_rows),
        main_table,
        dense_part,
        small_ids.reshape(1, examples),
        scale_ids.reshape(1, examples),
        small_table,
    )
    return jnp.transpose(result, (1, 0, 2))


def solution(mesh):
    placed = (
        P("shard", None),
        P("shard", None),
        P("shard", None),
        P("shard"),
        P("shard", None),
        P("shard"),
    )
    return jax.shard_map(
        local, mesh=mesh, in_specs=placed, out_specs=P("shard", None, None), check_vma=False
    )
```

```python
import functools

import jax
import jax.numpy as jnp
from jax import lax
from jax.experimental import pallas as pl
from jax.experimental.pallas import tpu as pltpu
from jax.sharding import PartitionSpec as P

MESH = pl.DeviceIdType.MESH
AXIS = "shard"
BATCH = 4


def two_terms(x):
    high = x.astype(jnp.bfloat16)
    low = (x - high.astype(jnp.float32)).astype(jnp.bfloat16)
    return high, low


def kernel(
    groups,
    picked_ref,
    table_ref,
    dense_ref,
    small_ids_ref,
    scale_ids_ref,
    small_ref,
    out_ref,
    ids_buf,
    table_buf,
    small_buf,
    dense_buf,
    lookup_buf,
    weights,
    counts,
    part_buf,
    recv_buf,
    local_sem,
    pair_send,
    pair_recv,
    ids_send,
    ids_recv,
    small_send,
    small_recv,
    part_send,
    part_recv,
):
    picks, examples = picked_ref.shape
    rows = table_ref.shape[0]
    small = small_ref.shape[0]
    batch = min(BATCH, groups)
    me = lax.axis_index(AXIS)
    core = lax.rem(me, 2)
    mine = lax.div(me, 2)
    partner = mine * 2 + 1 - core

    def peer(step):
        return lax.rem(mine + step + 1, groups)

    barrier = pltpu.get_barrier_semaphore()
    pl.semaphore_signal(barrier, inc=1, device_id=(partner,), device_id_type=MESH)

    def greet(step, _):
        pl.semaphore_signal(
            barrier, inc=1, device_id=(peer(step) * 2 + core,), device_id_type=MESH
        )
        return 0

    lax.fori_loop(0, groups - 1, greet, 0)

    own_rows = table_buf.at[pl.ds(pl.multiple_of(core * rows, rows), rows)]
    own_small = small_buf.at[pl.ds(pl.multiple_of(me * small, small), small)]
    ids_in = pltpu.make_async_copy(picked_ref, ids_buf.at[mine], local_sem.at[2])
    ids_in.start()
    table_in = pltpu.make_async_copy(table_ref, own_rows, local_sem.at[0])
    small_in = pltpu.make_async_copy(small_ref, own_small, local_sem.at[1])
    table_in.start()
    small_in.start()
    dense_in = pltpu.make_async_copy(dense_ref, dense_buf, local_sem.at[3])
    first_in = pltpu.make_async_copy(small_ids_ref, lookup_buf.at[0], local_sem.at[4])
    second_in = pltpu.make_async_copy(scale_ids_ref, lookup_buf.at[1], local_sem.at[5])
    dense_in.start()
    first_in.start()
    second_in.start()
    ids_in.wait()
    small_in.wait()
    pl.semaphore_wait(barrier, groups)

    def ids_copy(slot, sem, to):
        return pltpu.make_async_remote_copy(
            src_ref=ids_buf.at[slot],
            dst_ref=ids_buf.at[slot],
            send_sem=ids_send.at[sem],
            recv_sem=ids_recv.at[slot],
            device_id=(to * 2 + core,),
            device_id_type=MESH,
        )

    def send_ids(step, _):
        ids_copy(mine, step, peer(step)).start()
        return 0

    lax.fori_loop(0, groups - 1, send_ids, 0)

    def pair_copy(src, dst, sem):
        return pltpu.make_async_remote_copy(
            src_ref=src,
            dst_ref=dst,
            send_sem=pair_send.at[sem],
            recv_sem=pair_recv.at[sem],
            device_id=(partner,),
            device_id_type=MESH,
        )

    pair_small = pair_copy(own_small, own_small, 0)
    pair_small.start()
    table_in.wait()
    pair_table = pair_copy(own_rows, own_rows, 1)
    pair_table.start()
    pair_small.wait()

    def small_copy(slot, sem, to):
        block = small_buf.at[pl.ds(pl.multiple_of(slot * 2 * small, 2 * small), 2 * small)]
        return pltpu.make_async_remote_copy(
            src_ref=block,
            dst_ref=block,
            send_sem=small_send.at[sem],
            recv_sem=small_recv.at[slot],
            device_id=(to * 2 + core,),
            device_id_type=MESH,
        )

    def send_small(step, _):
        small_copy(mine, step, peer(step)).start()
        return 0

    lax.fori_loop(0, groups - 1, send_small, 0)

    pair_table.wait()
    high, low = two_terms(table_buf[...])
    features = high.shape[1]
    weights[:, :features] = high
    weights[:, features:] = low

    def part_copy(step, slot, to):
        return pltpu.make_async_remote_copy(
            src_ref=part_buf.at[pl.ds(pl.multiple_of(step * examples, examples), examples)],
            dst_ref=recv_buf.at[pl.ds(pl.multiple_of(slot * examples, examples), examples)],
            send_sem=part_send.at[step],
            recv_sem=part_recv.at[slot],
            device_id=(to * 2 + core,),
            device_id_type=MESH,
        )

    first = mine * (2 * rows)
    half = 16
    row_of = lax.broadcasted_iota(jnp.int32, (half, 2 * rows), 1)

    def serve(index, _):
        for q in range(batch):
            source = peer(index * batch + q)

            @pl.when(source != mine)
            def _():
                ids_copy(source, 0, source).wait_recv()

            wanted = jnp.transpose(ids_buf[source]) - first
            for h in range(examples // half):
                block = wanted[h * half : (h + 1) * half]
                count = jnp.zeros((half, 2 * rows), jnp.int32)
                for k in range(picks):
                    count = count + (block[:, k : k + 1] == row_of).astype(jnp.int32)
                counts[pl.ds(q * examples + h * half, half), :] = count.astype(
                    jnp.float32
                ).astype(jnp.bfloat16)
        both = jnp.dot(counts[...], weights[...], preferred_element_type=jnp.float32)
        total = both[:, :features] + both[:, features:]
        part_buf[
            pl.ds(pl.multiple_of(index * batch * examples, batch * examples), batch * examples), :
        ] = total
        for q in range(batch):
            step = index * batch + q
            to = peer(step)

            @pl.when(to != mine)
            def _():
                part_copy(step, mine, to).start()

        return 0

    lax.fori_loop(0, groups // batch, serve, 0)

    def take_small(step, _):
        source = peer(step)
        small_copy(source, 0, source).wait_recv()
        return 0

    lax.fori_loop(0, groups - 1, take_small, 0)

    all_small = small_buf.shape[0]
    small_row = lax.broadcasted_iota(jnp.int32, (all_small, examples), 0)
    table = small_buf[...]
    s_high, s_rest = table.astype(jnp.bfloat16), None
    rest = table - s_high.astype(jnp.float32)
    s_mid, s_low = two_terms(rest)

    def look_up(ids):
        chosen = jnp.where(ids == small_row, 1.0, 0.0).astype(jnp.bfloat16)

        def take(values):
            return lax.dot_general(
                chosen,
                values,
                (((0,), (0,)), ((), ())),
                preferred_element_type=jnp.float32,
            )

        return take(s_high) + take(s_mid) + take(s_low)

    dense_in.wait()
    first_in.wait()
    second_in.wait()
    small_rows = look_up(lookup_buf[0])
    dense = dense_buf[...] * look_up(lookup_buf[1])

    def add(step, total):
        source = lax.rem(mine + groups - 1 - step, groups)
        part_copy(0, source, source).wait_recv()
        return total + recv_buf[
            pl.ds(pl.multiple_of(source * examples, examples), examples), :
        ]

    total = lax.fori_loop(0, groups - 1, add, part_buf[(groups - 1) * examples :, :])
    pooled = total * picks ** (-0.5)
    out_ref[0] = dense * pooled
    out_ref[1] = pooled * small_rows
    out_ref[2] = dense * small_rows

    def finish(step, _):
        ids_copy(mine, step, peer(step)).wait_send()
        small_copy(mine, step, peer(step)).wait_send()
        part_copy(step, mine, peer(step)).wait_send()
        return 0

    lax.fori_loop(0, groups - 1, finish, 0)


def local(picked_rows, main_table, dense_part, small_ids, small_table, scale_ids):
    devices = lax.axis_size(AXIS)
    groups = devices // 2
    examples, picks = picked_rows.shape
    rows, features = main_table.shape
    small = small_table.shape[0]
    vmem = pl.BlockSpec(memory_space=pltpu.VMEM)
    anywhere = pl.BlockSpec(memory_space=pl.ANY)
    dma = pltpu.SemaphoreType.DMA
    result = pl.pallas_call(
        functools.partial(kernel, groups),
        out_shape=pltpu.VMEM((3, examples, features), jnp.float32),
        in_specs=[anywhere] * 6,
        out_specs=vmem,
        scratch_shapes=[
            pltpu.VMEM((groups, picks, examples), jnp.int32),
            pltpu.VMEM((2 * rows, features), jnp.float32),
            pltpu.VMEM((devices * small, features), jnp.float32),
            pltpu.VMEM((examples, features), jnp.float32),
            pltpu.VMEM((2, 1, examples), jnp.int32),
            pltpu.VMEM((2 * rows, 2 * features), jnp.bfloat16),
            pltpu.VMEM((min(BATCH, groups) * examples, 2 * rows), jnp.bfloat16),
            pltpu.VMEM((groups * examples, features), jnp.float32),
            pltpu.VMEM((groups * examples, features), jnp.float32),
            dma((6,)),
            dma((2,)),
            dma((2,)),
            dma((groups,)),
            dma((groups,)),
            dma((groups,)),
            dma((groups,)),
            dma((groups,)),
            dma((groups,)),
        ],
        compiler_params=pltpu.CompilerParams(collective_id=0, has_side_effects=True),
    )(
        jnp.transpose(picked_rows),
        main_table,
        dense_part,
        small_ids.reshape(1, examples),
        scale_ids.reshape(1, examples),
        small_table,
    )
    return jnp.transpose(result, (1, 0, 2))


def solution(mesh):
    placed = (
        P("shard", None),
        P("shard", None),
        P("shard", None),
        P("shard"),
        P("shard", None),
        P("shard"),
    )
    return jax.shard_map(
        local, mesh=mesh, in_specs=placed, out_specs=P("shard", None, None), check_vma=False
    )
```

```python
import functools

import jax
import jax.numpy as jnp
from jax import lax
from jax.experimental import pallas as pl
from jax.experimental.pallas import tpu as pltpu
from jax.sharding import PartitionSpec as P

MESH = pl.DeviceIdType.MESH
AXIS = "shard"
BATCH = 4


def two_terms(x):
    high = x.astype(jnp.bfloat16)
    low = (x - high.astype(jnp.float32)).astype(jnp.bfloat16)
    return high, low


def kernel(
    groups,
    picked_ref,
    table_ref,
    dense_ref,
    small_ids_ref,
    scale_ids_ref,
    small_ref,
    out_ref,
    ids_buf,
    table_buf,
    small_buf,
    dense_buf,
    lookup_buf,
    weights,
    counts,
    part_buf,
    recv_buf,
    local_sem,
    pair_send,
    pair_recv,
    ids_send,
    ids_recv,
    small_send,
    small_recv,
    part_send,
    part_recv,
):
    picks, examples = picked_ref.shape
    rows = table_ref.shape[0]
    small = small_ref.shape[0]
    batch = min(BATCH, groups)
    me = lax.axis_index(AXIS)
    core = lax.rem(me, 2)
    mine = lax.div(me, 2)
    partner = mine * 2 + 1 - core

    within = lax.rem(mine, batch)
    base = mine - within

    def peer(step):
        block = lax.div(step, batch)
        side = 1 - 2 * lax.rem(block + 1, 2)
        start = jnp.where(block == 0, 0, groups // 2 + side * batch * lax.div(block, 2))
        return lax.rem(base + start, groups) + lax.rem(within + step, batch)

    def far_first(index):
        return 1 + lax.rem(index + batch - 1, groups - 1)

    barrier = pltpu.get_barrier_semaphore()
    pl.semaphore_signal(barrier, inc=1, device_id=(partner,), device_id_type=MESH)

    def greet(index, _):
        step = far_first(index)
        pl.semaphore_signal(
            barrier, inc=1, device_id=(peer(step) * 2 + core,), device_id_type=MESH
        )
        return 0

    lax.fori_loop(0, groups - 1, greet, 0)

    own_rows = table_buf.at[pl.ds(pl.multiple_of(core * rows, rows), rows)]
    own_small = small_buf.at[pl.ds(pl.multiple_of(me * small, small), small)]
    ids_in = pltpu.make_async_copy(picked_ref, ids_buf.at[mine], local_sem.at[2])
    ids_in.start()
    table_in = pltpu.make_async_copy(table_ref, own_rows, local_sem.at[0])
    small_in = pltpu.make_async_copy(small_ref, own_small, local_sem.at[1])
    table_in.start()
    small_in.start()
    dense_in = pltpu.make_async_copy(dense_ref, dense_buf, local_sem.at[3])
    first_in = pltpu.make_async_copy(small_ids_ref, lookup_buf.at[0], local_sem.at[4])
    second_in = pltpu.make_async_copy(scale_ids_ref, lookup_buf.at[1], local_sem.at[5])
    dense_in.start()
    first_in.start()
    second_in.start()
    ids_in.wait()
    small_in.wait()
    pl.semaphore_wait(barrier, groups)

    def ids_copy(slot, sem, to):
        return pltpu.make_async_remote_copy(
            src_ref=ids_buf.at[slot],
            dst_ref=ids_buf.at[slot],
            send_sem=ids_send.at[sem],
            recv_sem=ids_recv.at[slot],
            device_id=(to * 2 + core,),
            device_id_type=MESH,
        )

    def send_ids(index, _):
        step = far_first(index)
        ids_copy(mine, step, peer(step)).start()
        return 0

    lax.fori_loop(0, groups - 1, send_ids, 0)

    def pair_copy(src, dst, sem):
        return pltpu.make_async_remote_copy(
            src_ref=src,
            dst_ref=dst,
            send_sem=pair_send.at[sem],
            recv_sem=pair_recv.at[sem],
            device_id=(partner,),
            device_id_type=MESH,
        )

    pair_small = pair_copy(own_small, own_small, 0)
    pair_small.start()
    table_in.wait()
    pair_table = pair_copy(own_rows, own_rows, 1)
    pair_table.start()
    pair_small.wait()

    def small_copy(slot, sem, to):
        block = small_buf.at[pl.ds(pl.multiple_of(slot * 2 * small, 2 * small), 2 * small)]
        return pltpu.make_async_remote_copy(
            src_ref=block,
            dst_ref=block,
            send_sem=small_send.at[sem],
            recv_sem=small_recv.at[slot],
            device_id=(to * 2 + core,),
            device_id_type=MESH,
        )

    def send_small(step, _):
        small_copy(mine, step, peer(step)).start()
        return 0

    lax.fori_loop(1, groups, send_small, 0)

    pair_table.wait()
    high, low = two_terms(table_buf[...])
    features = high.shape[1]
    weights[:, :features] = high
    weights[:, features:] = low

    def part_copy(step, slot, to):
        return pltpu.make_async_remote_copy(
            src_ref=part_buf.at[pl.ds(pl.multiple_of(step * examples, examples), examples)],
            dst_ref=recv_buf.at[pl.ds(pl.multiple_of(slot * examples, examples), examples)],
            send_sem=part_send.at[step],
            recv_sem=part_recv.at[slot],
            device_id=(to * 2 + core,),
            device_id_type=MESH,
        )

    first = mine * (2 * rows)
    half = 16
    row_of = lax.broadcasted_iota(jnp.int32, (half, 2 * rows), 1)

    def serve(index, _):
        for q in range(batch):
            source = peer(index * batch + q)

            @pl.when(source != mine)
            def _():
                ids_copy(source, 0, source).wait_recv()

            wanted = jnp.transpose(ids_buf[source]) - first
            for h in range(examples // half):
                block = wanted[h * half : (h + 1) * half]
                count = jnp.zeros((half, 2 * rows), jnp.int32)
                for k in range(picks):
                    count = count + (block[:, k : k + 1] == row_of).astype(jnp.int32)
                counts[pl.ds(q * examples + h * half, half), :] = count.astype(
                    jnp.float32
                ).astype(jnp.bfloat16)
        both = jnp.dot(counts[...], weights[...], preferred_element_type=jnp.float32)
        total = both[:, :features] + both[:, features:]
        part_buf[
            pl.ds(pl.multiple_of(index * batch * examples, batch * examples), batch * examples), :
        ] = total
        for q in range(batch):
            step = index * batch + q
            to = peer(step)

            @pl.when(to != mine)
            def _():
                part_copy(step, mine, to).start()

        return 0

    lax.fori_loop(0, groups // batch, serve, 0)

    def take_small(step, _):
        source = peer(step)
        small_copy(source, 0, source).wait_recv()
        return 0

    lax.fori_loop(1, groups, take_small, 0)

    all_small = small_buf.shape[0]
    small_row = lax.broadcasted_iota(jnp.int32, (all_small, examples), 0)
    table = small_buf[...]
    s_high, s_rest = table.astype(jnp.bfloat16), None
    rest = table - s_high.astype(jnp.float32)
    s_mid, s_low = two_terms(rest)

    def look_up(ids):
        chosen = jnp.where(ids == small_row, 1.0, 0.0).astype(jnp.bfloat16)

        def take(values):
            return lax.dot_general(
                chosen,
                values,
                (((0,), (0,)), ((), ())),
                preferred_element_type=jnp.float32,
            )

        return take(s_high) + take(s_mid) + take(s_low)

    dense_in.wait()
    first_in.wait()
    second_in.wait()
    small_rows = look_up(lookup_buf[0])
    dense = dense_buf[...] * look_up(lookup_buf[1])

    def add(step, total):
        source = peer(step)
        part_copy(0, source, source).wait_recv()
        return total + recv_buf[
            pl.ds(pl.multiple_of(source * examples, examples), examples), :
        ]

    total = lax.fori_loop(1, groups, add, part_buf[:examples, :])
    pooled = total * picks ** (-0.5)
    out_ref[0] = dense * pooled
    out_ref[1] = pooled * small_rows
    out_ref[2] = dense * small_rows

    def finish(step, _):
        ids_copy(mine, step, peer(step)).wait_send()
        small_copy(mine, step, peer(step)).wait_send()
        part_copy(step, mine, peer(step)).wait_send()
        return 0

    lax.fori_loop(1, groups, finish, 0)


def local(picked_rows, main_table, dense_part, small_ids, small_table, scale_ids):
    devices = lax.axis_size(AXIS)
    groups = devices // 2
    examples, picks = picked_rows.shape
    rows, features = main_table.shape
    small = small_table.shape[0]
    vmem = pl.BlockSpec(memory_space=pltpu.VMEM)
    anywhere = pl.BlockSpec(memory_space=pl.ANY)
    dma = pltpu.SemaphoreType.DMA
    result = pl.pallas_call(
        functools.partial(kernel, groups),
        out_shape=pltpu.VMEM((3, examples, features), jnp.float32),
        in_specs=[anywhere] * 6,
        out_specs=vmem,
        scratch_shapes=[
            pltpu.VMEM((groups, picks, examples), jnp.int32),
            pltpu.VMEM((2 * rows, features), jnp.float32),
            pltpu.VMEM((devices * small, features), jnp.float32),
            pltpu.VMEM((examples, features), jnp.float32),
            pltpu.VMEM((2, 1, examples), jnp.int32),
            pltpu.VMEM((2 * rows, 2 * features), jnp.bfloat16),
            pltpu.VMEM((min(BATCH, groups) * examples, 2 * rows), jnp.bfloat16),
            pltpu.VMEM((groups * examples, features), jnp.float32),
            pltpu.VMEM((groups * examples, features), jnp.float32),
            dma((6,)),
            dma((2,)),
            dma((2,)),
            dma((groups,)),
            dma((groups,)),
            dma((groups,)),
            dma((groups,)),
            dma((groups,)),
            dma((groups,)),
        ],
        compiler_params=pltpu.CompilerParams(collective_id=0, has_side_effects=True),
    )(
        jnp.transpose(picked_rows),
        main_table,
        dense_part,
        small_ids.reshape(1, examples),
        scale_ids.reshape(1, examples),
        small_table,
    )
    return jnp.transpose(result, (1, 0, 2))


def solution(mesh):
    placed = (
        P("shard", None),
        P("shard", None),
        P("shard", None),
        P("shard"),
        P("shard", None),
        P("shard"),
    )
    return jax.shard_map(
        local, mesh=mesh, in_specs=placed, out_specs=P("shard", None, None), check_vma=False
    )
```
